32 devices in a mesh: bngroup: 4 (over z), rep: 8 (over y, x, core).
Axes of the slice: x: 2, y: 2, z: 4, core: 2. Of those that a mesh axis runs over, the one named last changes fastest.
Arguments:
- images: bfloat16 [384, 7, 7, 2048], P(('bngroup', 'rep')), may hold values from -12 to 12
- cotangent: bfloat16 [384, 7, 7, 2048], P(('bngroup', 'rep')), may hold values from -6 to 6
- w_reduce: bfloat16 [2048, 512], replicated, may hold values from -0.125 to 0.125
- w_spatial: bfloat16 [4608, 512], replicated, may hold values from -0.09375 to 0.09375
- w_expand: bfloat16 [2048, 512], replicated, may hold values from -0.25 to 0.25
- norm_gain: float32 [3072], replicated, may hold values from 0.25 to 1.75
- norm_shift: float32 [3072], replicated, may hold values from -3 to 3
Outputs:
- output: bfloat16 [384, 7, 7, 2048], P(('bngroup', 'rep'))
- in_grad: bfloat16 [384, 7, 7, 2048], P(('bngroup', 'rep'))
- weight_grads: float32 [8704, 512], P('bngroup', 'rep')
- norm_grads: float32 [2, 3072], replicated
The draws below stay inside these ranges and needn't reach their ends.
All inputs are finite; a program needn't handle non-finite values.
Results may differ from the reference program's by a relative error of at most 0.007.
Values sent between devices are 32-bit elements.
A program may use at most 192 MiB of HBM per device.

```python
import jax
import jax.numpy as jnp
from jax import lax

WIDE = 2048
MID = 512
SIDE = 7
IMG_DEV = 12
IMAGES = 384
NORM_CH = 3072
N_BNGROUP = 4
N_REP = 8


def draw_images(key, part):
    base_key, scale_key = jax.random.split(jax.random.fold_in(key, 11))
    values = jnp.clip(jax.random.normal(base_key, (IMAGES, SIDE, SIDE, WIDE), jnp.float32), -6.0, 6.0)
    scales = jnp.exp(jax.random.uniform(scale_key, (IMAGES, 1, 1, 1), jnp.float32, -0.69, 0.69))
    return (values * scales).astype(jnp.bfloat16)


def block_scale(stream_key, shape, shards, smallest, high):
    factor_of, own = 1.0, jax.random.fold_in(stream_key, 6)
    for axis_at, shards_of in shards:
        draws = jnp.exp(jax.random.uniform(jax.random.fold_in(own, axis_at), (shards_of,), jnp.float32, smallest / len(shards), high / len(shards)))
        factor_of = factor_of * jnp.repeat(draws, shape[axis_at] // shards_of).reshape([-1 if axis == axis_at else 1 for axis in range(len(shape))])
    return factor_of


def bell_draw(stream_key, extent, scale, bound, shards=(), kind=jnp.bfloat16):
    values = jax.random.normal(stream_key, extent, jnp.float32) * scale
    if len(shards) > 0:
        values = block_scale(stream_key, extent, shards, -0.22, 0.18) * values
    return jnp.clip(values, min=-bound, max=bound).astype(kind)


def setup_inputs(seed: int = 0) -> dict:
    seeds = jax.random.split(jax.random.key(seed), 8)
    return {
        "images": draw_images(jax.random.fold_in(seeds[7], 71), 0),
        "cotangent": bell_draw(seeds[1], (IMAGES, SIDE, SIDE, WIDE), 1.0, 6.0, ((0, 32),)),
        "w_reduce": bell_draw(seeds[2], (WIDE, MID), WIDE ** -0.5, 0.125),
        "w_spatial": bell_draw(seeds[3], (9 * MID, MID), (9 * MID) ** -0.5, 0.09375),
        "w_expand": bell_draw(seeds[4], (WIDE, MID), MID ** -0.5, 0.25),
        "norm_gain": jnp.clip(1.0 + 0.15 * jax.random.normal(seeds[5], (NORM_CH,), jnp.float32), 0.25, 1.75),
        "norm_shift": bell_draw(seeds[6], (NORM_CH,), 0.5, 3.0, (), jnp.float32),
    }


EPS = 0.25

def matmul(left, right):
    return jnp.dot(left, right, preferred_element_type=jnp.float32)

def contract(left, right, left_dim, right_dim):
    return lax.dot_general(left, right, (((left_dim,), (right_dim,)), ((), ())), preferred_element_type=jnp.float32)

def slope(value):
    sigma = jax.nn.sigmoid(value)
    return sigma * (1.0 + value * (1.0 - sigma))

def normalize(pre_norm, norm_gain, norm_shift):
    centre = lax.optimization_barrier(jnp.mean(pre_norm, axis=0))
    spread = lax.optimization_barrier(jnp.mean(jnp.square(pre_norm - centre), axis=0))
    inverse = lax.rsqrt(spread + EPS)
    scaled = (pre_norm - centre) * inverse
    return (scaled, inverse, norm_gain * scaled + norm_shift)

def norm_back(upstream, scaled, inverse, norm_gain):
    shift_sum = lax.optimization_barrier(jnp.sum(upstream, axis=0))
    gain_sum = lax.optimization_barrier(jnp.sum(upstream * scaled, axis=0))
    number = upstream.shape[0]
    result = norm_gain * inverse * (upstream - shift_sum / number - scaled * gain_sum / number)
    return (result.astype(jnp.bfloat16), shift_sum, gain_sum)

def unfold(field):
    length = field.shape[1]
    padded = jnp.pad(field, ((0, 0), (1, 1), (1, 1), (0, 0)))
    windows = [padded[:, row_tap:row_tap + length, col_tap:col_tap + length, :] for row_tap in range(3) for col_tap in range(3)]
    return jnp.concatenate(windows, axis=-1).reshape(-1, 9 * field.shape[3])

def fold_back(columns, images_count, length, channels):
    shaped = columns.reshape(images_count, length, length, 9, channels)
    summed = jnp.zeros((images_count, length + 2, length + 2, channels), jnp.float32)
    for row_tap in range(3):
        for col_tap in range(3):
            summed = summed + jnp.pad(shaped[:, :, :, 3 * row_tap + col_tap, :], ((0, 0), (row_tap, 2 - row_tap), (col_tap, 2 - col_tap), (0, 0)))
    return summed[:, 1:length + 1, 1:length + 1, :].reshape(-1, channels)

def block_pass(images, cotangent, w_reduce, w_spatial, w_expand, norm_gain, norm_shift):
    images_count = images.shape[0]
    length = images.shape[1]
    wide_ch = images.shape[3]
    mid_ch = w_reduce.shape[1]
    flat_in = images.reshape(-1, wide_ch)
    gain_one, gain_two, gain_three = (norm_gain[:mid_ch], norm_gain[mid_ch:2 * mid_ch], norm_gain[2 * mid_ch:])
    shift_one, shift_two, shift_three = (norm_shift[:mid_ch], norm_shift[mid_ch:2 * mid_ch], norm_shift[2 * mid_ch:])
    scaled_one, inverse_one, normed_one = normalize(matmul(flat_in, w_reduce), gain_one, shift_one)
    hidden_one = jax.nn.silu(normed_one).astype(jnp.bfloat16)
    patches = unfold(hidden_one.reshape(images_count, length, length, mid_ch))
    scaled_two, inverse_two, normed_two = normalize(matmul(patches, w_spatial), gain_two, shift_two)
    hidden_two = jax.nn.silu(normed_two).astype(jnp.bfloat16)
    scaled_three, inverse_three, normed_three = normalize(contract(hidden_two, w_expand, 1, 1), gain_three, shift_three)
    summed_in = normed_three + flat_in.astype(jnp.float32)
    output = jax.nn.silu(summed_in).astype(jnp.bfloat16)
    upstream = cotangent.reshape(-1, wide_ch).astype(jnp.float32) * slope(summed_in)
    grad_three, shift_sum_three, gain_sum_three = norm_back(upstream, scaled_three, inverse_three, gain_three)
    back_two = matmul(grad_three, w_expand) * slope(normed_two)
    grad_two, shift_sum_two, gain_sum_two = norm_back(back_two, scaled_two, inverse_two, gain_two)
    back_one = fold_back(contract(grad_two, w_spatial, 1, 1), images_count, length, mid_ch) * slope(normed_one)
    grad_one, shift_sum_one, gain_sum_one = norm_back(back_one, scaled_one, inverse_one, gain_one)
    in_grad = (upstream + contract(grad_one, w_reduce, 1, 1)).astype(jnp.bfloat16)
    weight_grads = jnp.concatenate([contract(flat_in, grad_one, 0, 0), contract(patches, grad_two, 0, 0), contract(grad_three, hidden_two, 0, 0)], axis=0)
    norm_grads = jnp.stack([jnp.concatenate([gain_sum_one, gain_sum_two, gain_sum_three]), jnp.concatenate([shift_sum_one, shift_sum_two, shift_sum_three])])
    return (output.reshape(images.shape), in_grad.reshape(images.shape), weight_grads, norm_grads)

def reference(images, cotangent, w_reduce, w_spatial, w_expand, norm_gain, norm_shift):

    def regroup(array):
        tail = array.shape[1:]
        return array.reshape((N_BNGROUP, N_REP, IMG_DEV) + tail).swapaxes(0, 1).reshape((N_REP, N_BNGROUP * IMG_DEV) + tail)

    def ungroup(array):
        tail = array.shape[2:]
        return array.reshape((N_REP, N_BNGROUP, IMG_DEV) + tail).swapaxes(0, 1).reshape((IMAGES,) + tail)

    def group_step(totals, group_items):
        output, in_grad, weight_part, norm_part = block_pass(group_items[0], group_items[1], w_reduce, w_spatial, w_expand, norm_gain, norm_shift)
        return ((totals[0] + weight_part, totals[1] + norm_part), (output, in_grad))
    start_totals = (jnp.zeros((2 * WIDE + 9 * MID, MID), jnp.float32), jnp.zeros((2, 2 * MID + WIDE), jnp.float32))
    totals, results = lax.scan(group_step, start_totals, (regroup(images), regroup(cotangent)))
    return (ungroup(results[0]), ungroup(results[1]), totals[0] / IMAGES, totals[1] / IMAGES)
```

```python
import functools

import jax
import jax.numpy as jnp
from jax import lax
from jax.experimental import pallas as pl
from jax.experimental.pallas import tpu as pltpu
from jax.sharding import PartitionSpec as P

MESH = pl.DeviceIdType.MESH

EPS = 0.25


def matmul(left, right):
    return jnp.dot(left, right, preferred_element_type=jnp.float32)


def contract(left, right, left_dim, right_dim):
    return lax.dot_general(
        left, right, (((left_dim,), (right_dim,)), ((), ())), preferred_element_type=jnp.float32
    )


def exchange_kernel(axis, size, value_ref, total_ref, slots, send_sem, recv_sem):
    me = lax.axis_index(axis)
    barrier = pltpu.get_barrier_semaphore()
    for step in range(1, size):
        peer = lax.rem(me + step, size)
        pl.semaphore_signal(barrier, inc=1, device_id={axis: peer}, device_id_type=MESH)
    pl.semaphore_wait(barrier, size - 1)
    copies = []
    for step in range(1, size):
        peer = lax.rem(me + step, size)
        copy = pltpu.make_async_remote_copy(
            src_ref=value_ref,
            dst_ref=slots.at[me],
            send_sem=send_sem.at[step],
            recv_sem=recv_sem.at[step],
            device_id={axis: peer},
            device_id_type=MESH,
        )
        copy.start()
        copies.append(copy)
    slots[me] = value_ref[...]
    for copy in copies:
        copy.wait()
    total = slots[0]
    for member in range(1, size):
        total = total + slots[member]
    total_ref[...] = total


def exchange_sum(value, axis, ident):
    size = lax.axis_size(axis)
    return pl.pallas_call(
        functools.partial(exchange_kernel, axis, size),
        out_shape=jax.ShapeDtypeStruct(value.shape, value.dtype),
        in_specs=[pl.BlockSpec(memory_space=pltpu.VMEM)],
        out_specs=pl.BlockSpec(memory_space=pltpu.VMEM),
        scratch_shapes=[
            pltpu.VMEM((size,) + value.shape, value.dtype),
            pltpu.SemaphoreType.DMA((size,)),
            pltpu.SemaphoreType.DMA((size,)),
        ],
        compiler_params=pltpu.CompilerParams(collective_id=ident, has_side_effects=True),
        name="exchange_" + str(ident),
    )(value)


def weight_kernel(starts, grad_one, flat_in, grad_two, patches, hidden_two, grad_three, out_ref):
    at = pl.program_id(0)

    @pl.when(at < starts[0])
    def _():
        out_ref[...] = contract(grad_one[...], flat_in[...], 0, 0)

    @pl.when(jnp.logical_and(at >= starts[0], at < starts[1]))
    def _():
        out_ref[...] = contract(grad_two[...], patches[...], 0, 0)

    @pl.when(at >= starts[1])
    def _():
        out_ref[...] = contract(hidden_two[...], grad_three[...], 0, 0)


def weight_products(grad_one, flat_in, grad_two, patches, hidden_two, grad_three):
    rows, mid = grad_one.shape
    counts = [array.shape[1] // mid for array in (flat_in, patches, grad_three)]
    starts = (counts[0], counts[0] + counts[1])
    whole = pl.BlockSpec((rows, mid), lambda at: (0, 0))

    def columns(first, count):
        return pl.BlockSpec((rows, mid), lambda at: (0, jnp.clip(at - first, 0, count - 1)))

    return pl.pallas_call(
        functools.partial(weight_kernel, starts),
        grid=(sum(counts),),
        out_shape=jax.ShapeDtypeStruct((mid, sum(counts) * mid), jnp.float32),
        in_specs=[
            whole,
            columns(0, counts[0]),
            whole,
            columns(starts[0], counts[1]),
            whole,
            columns(starts[1], counts[2]),
        ],
        out_specs=pl.BlockSpec((mid, mid), lambda at: (0, at)),
        name="weight_products",
    )(grad_one, flat_in, grad_two, patches, hidden_two, grad_three)


def scatter_plan(n_group, n_rep, rows):
    bits = [("rep", at) for at in range(n_rep.bit_length() - 1)]
    bits += [("bngroup", at) for at in range(n_group.bit_length() - 1)]
    rest = len(bits) - 1
    near = list(range(rest))
    rep_rest = n_rep.bit_length() - 2
    orders = [
        near,
        near[1:rep_rest] + near[rep_rest:] + near[:1],
        near[rep_rest:] + near[:rep_rest],
    ]
    tiles = rows // 8
    sizes = [(tiles + 2) // 3, (tiles + 1) // 3, tiles // 3]
    streams, begin = [], 0
    for order, size in zip(orders, sizes):
        if size:
            streams.append((begin * 8, size * 8, order))
        begin += size
    return bits, streams


def scatter_kernel(n_group, n_rep, scale, grads, out_ref, own, got, load_sem, send_sem, recv_sem):
    rows, cols = out_ref.shape
    bits, streams = scatter_plan(n_group, n_rep, rows)
    rest = bits[1:]
    place = {"rep": lax.axis_index("rep"), "bngroup": lax.axis_index("bngroup")}

    def flipped(value, at):
        bit = lax.rem(value // (1 << at), 2)
        return value + (1 - 2 * bit) * (1 << at)

    def partner(axis, at):
        return {axis: flipped(place[axis], at)}

    barrier = pltpu.get_barrier_semaphore()
    for axis, at in bits:
        pl.semaphore_signal(barrier, inc=1, device_id=partner(axis, at), device_id_type=MESH)

    def source(relative, other, begin, size):
        spot = dict(place)
        for index, (axis, at) in enumerate(rest):
            if relative >> index & 1:
                spot[axis] = flipped(spot[axis], at)
        if other:
            spot["rep"] = flipped(spot["rep"], 0)
        first = pl.multiple_of(spot["rep"] * rows + begin, 8)
        if len(grads.shape) == 3:
            return grads.at[spot["bngroup"], pl.ds(first, size), :]
        return grads.at[pl.ds(first, size), pl.ds(pl.multiple_of(spot["bngroup"] * cols, 128), cols)]

    count = 1 << len(rest)
    slot_of, slots = {}, count
    for number, (begin, size, order) in enumerate(streams):
        used = count
        active = list(range(count))
        for stage, bit in enumerate(order):
            active = [relative for relative in active if not relative >> bit & 1]
            for relative in active:
                slot_of[number, stage, relative] = used
                used += 1

    def first_order(order):
        ranks = sorted(range(count), key=lambda rel: tuple(-(rel >> bit & 1) for bit in order))
        return ranks

    loads = {}
    for number, (begin, size, order) in enumerate(streams):
        for relative in range(count):
            copy = pltpu.make_async_copy(
                source(relative, False, begin, size),
                own.at[relative, pl.ds(begin, size), :],
                load_sem.at[number, relative],
            )
            loads[number, relative] = copy
    for relative in range(count):
        for number, (begin, size, order) in enumerate(streams):
            loads[number, first_order(order)[relative]].start()
    pl.semaphore_wait(barrier, len(bits))
    sent = []
    arrivals = {}
    for relative in range(count):
        for number, (begin, size, order) in enumerate(streams):
            which = first_order(order)[relative]
            copy = pltpu.make_async_remote_copy(
                src_ref=source(which, True, begin, size),
                dst_ref=got.at[which, pl.ds(begin, size), :],
                send_sem=send_sem.at[number, which],
                recv_sem=recv_sem.at[number, which],
                device_id=partner(*bits[0]),
                device_id_type=MESH,
            )
            copy.start()
            sent.append(copy)
            arrivals[number, -1, which] = copy

    def onward(number, stage, relative):
        begin, size, order = streams[number]
        bit = order[stage]
        slot = slot_of[number, stage, relative & ~(1 << bit)]
        copy = pltpu.make_async_remote_copy(
            src_ref=own.at[relative, pl.ds(begin, size), :],
            dst_ref=got.at[slot, pl.ds(begin, size), :],
            send_sem=send_sem.at[number, slot],
            recv_sem=recv_sem.at[number, slot],
            device_id=partner(*rest[bit]),
            device_id_type=MESH,
        )
        copy.start()
        sent.append(copy)
        arrivals[number, stage, relative & ~(1 << bit)] = copy

    pending = []
    for stage in range(-1, len(rest)):
        active = []
        for number, (begin, size, order) in enumerate(streams):
            done = 0
            for bit in order[: stage + 1]:
                done |= 1 << bit
            active.append([rel for rel in first_order(order) if not rel & done])
        for position in range(len(active[0])):
            for number, (begin, size, order) in enumerate(streams):
                relative = active[number][position]
                slot = relative if stage < 0 else slot_of[number, stage, relative]
                if stage < 0:
                    loads[number, relative].wait()
                arrivals[number, stage, relative].wait_recv()
                window = pl.ds(begin, size)
                total = own[relative, window, :] + got[slot, window, :]
                if stage == len(rest) - 1:
                    out_ref[window, :] = total * scale
                else:
                    own[relative, window, :] = total
                while pending:
                    onward(*pending.pop(0))
                if stage + 1 < len(rest) and relative >> order[stage + 1] & 1:
                    pending.append((number, stage + 1, relative))
        while pending:
            onward(*pending.pop(0))
    for copy in sent:
        copy.wait_send()


def scatter_sum(grads, images_total, ident):
    n_group, n_rep = lax.axis_size("bngroup"), lax.axis_size("rep")
    rows, cols = grads.shape[0] // n_rep, grads.shape[1] // n_group
    if cols % 128:
        grads = grads.reshape(grads.shape[0], n_group, cols).transpose(1, 0, 2)
    bits, streams = scatter_plan(n_group, n_rep, rows)
    count = 1 << (len(bits) - 1)
    held = 2 * count - 1
    return pl.pallas_call(
        functools.partial(scatter_kernel, n_group, n_rep, 1.0 / images_total),
        out_shape=jax.ShapeDtypeStruct((rows, cols), jnp.float32),
        in_specs=[pl.BlockSpec(memory_space=pl.ANY)],
        out_specs=pl.BlockSpec(memory_space=pltpu.VMEM),
        scratch_shapes=[
            pltpu.VMEM((count, rows, cols), jnp.float32),
            pltpu.VMEM((held, rows, cols), jnp.float32),
            pltpu.SemaphoreType.DMA((len(streams), count)),
            pltpu.SemaphoreType.DMA((len(streams), held)),
            pltpu.SemaphoreType.DMA((len(streams), held)),
        ],
        compiler_params=pltpu.CompilerParams(
            collective_id=ident, has_side_effects=True, vmem_limit_bytes=60 * 1024 * 1024
        ),
        name="scatter_sum",
    )(grads)


def slope(value):
    sigma = jax.nn.sigmoid(value)
    return sigma * (1.0 + value * (1.0 - sigma))


def normalize(pre_norm, norm_gain, norm_shift, group_size, ident):
    number = pre_norm.shape[0] * group_size
    sums = jnp.stack([jnp.sum(pre_norm, axis=0), jnp.sum(pre_norm * pre_norm, axis=0)])
    first_sum, second_sum = exchange_sum(sums, "bngroup", ident)
    centre = first_sum / number
    spread = jnp.maximum(second_sum / number - centre * centre, 0.0)
    inverse = lax.rsqrt(spread + EPS)
    scaled = (pre_norm - centre) * inverse
    return (scaled, inverse, norm_gain * scaled + norm_shift)


def norm_back(upstream, scaled, inverse, norm_gain, group_size, ident):
    sums = jnp.stack([jnp.sum(upstream, axis=0), jnp.sum(upstream * scaled, axis=0)])
    shift_sum, gain_sum = exchange_sum(sums, "bngroup", ident)
    number = upstream.shape[0] * group_size
    result = norm_gain * inverse * (upstream - shift_sum / number - scaled * gain_sum / number)
    return (result.astype(jnp.bfloat16), shift_sum, gain_sum)


def unfold(field):
    length = field.shape[1]
    padded = jnp.pad(field, ((0, 0), (1, 1), (1, 1), (0, 0)))
    windows = [
        padded[:, row_tap : row_tap + length, col_tap : col_tap + length, :]
        for row_tap in range(3)
        for col_tap in range(3)
    ]
    return jnp.concatenate(windows, axis=-1).reshape(-1, 9 * field.shape[3])


def fold_back(columns, images_count, length, channels):
    shaped = columns.reshape(images_count, length, length, 9, channels)
    summed = jnp.zeros((images_count, length + 2, length + 2, channels), jnp.float32)
    for row_tap in range(3):
        for col_tap in range(3):
            summed = summed + jnp.pad(
                shaped[:, :, :, 3 * row_tap + col_tap, :],
                ((0, 0), (row_tap, 2 - row_tap), (col_tap, 2 - col_tap), (0, 0)),
            )
    return summed[:, 1 : length + 1, 1 : length + 1, :].reshape(-1, channels)


def per_device(images, cotangent, w_reduce, w_spatial, w_expand, norm_gain, norm_shift):
    group_size = lax.axis_size("bngroup")
    images_total = images.shape[0] * group_size * lax.axis_size("rep")
    images_count = images.shape[0]
    length = images.shape[1]
    wide_ch = images.shape[3]
    mid_ch = w_reduce.shape[1]
    flat_in = images.reshape(-1, wide_ch)
    gain_one, gain_two, gain_three = (
        norm_gain[:mid_ch],
        norm_gain[mid_ch : 2 * mid_ch],
        norm_gain[2 * mid_ch :],
    )
    shift_one, shift_two, shift_three = (
        norm_shift[:mid_ch],
        norm_shift[mid_ch : 2 * mid_ch],
        norm_shift[2 * mid_ch :],
    )
    scaled_one, inverse_one, normed_one = normalize(
        matmul(flat_in, w_reduce), gain_one, shift_one, group_size, 0
    )
    hidden_one = jax.nn.silu(normed_one).astype(jnp.bfloat16)
    patches = unfold(hidden_one.reshape(images_count, length, length, mid_ch))
    scaled_two, inverse_two, normed_two = normalize(
        matmul(patches, w_spatial), gain_two, shift_two, group_size, 1
    )
    hidden_two = jax.nn.silu(normed_two).astype(jnp.bfloat16)
    scaled_three, inverse_three, normed_three = normalize(
        contract(hidden_two, w_expand, 1, 1), gain_three, shift_three, group_size, 2
    )
    summed_in = normed_three + flat_in.astype(jnp.float32)
    output = jax.nn.silu(summed_in).astype(jnp.bfloat16)
    upstream = cotangent.reshape(-1, wide_ch).astype(jnp.float32) * slope(summed_in)
    grad_three, shift_sum_three, gain_sum_three = norm_back(
        upstream, scaled_three, inverse_three, gain_three, group_size, 3
    )
    back_two = matmul(grad_three, w_expand) * slope(normed_two)
    grad_two, shift_sum_two, gain_sum_two = norm_back(
        back_two, scaled_two, inverse_two, gain_two, group_size, 4
    )
    back_one = fold_back(contract(grad_two, w_spatial, 1, 1), images_count, length, mid_ch) * slope(
        normed_one
    )
    grad_one, shift_sum_one, gain_sum_one = norm_back(
        back_one, scaled_one, inverse_one, gain_one, group_size, 5
    )
    in_grad = (upstream + contract(grad_one, w_reduce, 1, 1)).astype(jnp.bfloat16)
    local_grads = weight_products(
        grad_one, flat_in, grad_two, patches, hidden_two, grad_three
    )
    summed_grads = scatter_sum(local_grads, images_total, 7).T
    group_norms = jnp.stack(
        [
            jnp.concatenate([gain_sum_one, gain_sum_two, gain_sum_three]),
            jnp.concatenate([shift_sum_one, shift_sum_two, shift_sum_three]),
        ]
    )
    norm_summed = exchange_sum(group_norms, "rep", 6)
    return (
        output.reshape(images.shape),
        in_grad.reshape(images.shape),
        summed_grads,
        norm_summed / images_total,
    )


def solution(mesh):
    in_specs = (
        P(("bngroup", "rep"), None, None, None),
        P(("bngroup", "rep"), None, None, None),
        P(),
        P(),
        P(),
        P(),
        P(),
    )
    out_specs = (
        P(("bngroup", "rep"), None, None, None),
        P(("bngroup", "rep"), None, None, None),
        P("bngroup", "rep"),
        P(),
    )
    return jax.shard_map(
        per_device, mesh=mesh, in_specs=in_specs, out_specs=out_specs, check_vma=False
    )
```

```python
import functools

import jax
import jax.numpy as jnp
from jax import lax
from jax.experimental import pallas as pl
from jax.experimental.pallas import tpu as pltpu
from jax.sharding import PartitionSpec as P

MESH = pl.DeviceIdType.MESH

EPS = 0.25


def matmul(left, right):
    return jnp.dot(left, right, preferred_element_type=jnp.float32)


def contract(left, right, left_dim, right_dim):
    return lax.dot_general(
        left, right, (((left_dim,), (right_dim,)), ((), ())), preferred_element_type=jnp.float32
    )


def exchange_kernel(axis, size, value_ref, total_ref, slots, send_sem, recv_sem):
    me = lax.axis_index(axis)
    barrier = pltpu.get_barrier_semaphore()
    for step in range(1, size):
        peer = lax.rem(me + step, size)
        pl.semaphore_signal(barrier, inc=1, device_id={axis: peer}, device_id_type=MESH)
    pl.semaphore_wait(barrier, size - 1)
    copies = []
    for step in range(1, size):
        peer = lax.rem(me + step, size)
        copy = pltpu.make_async_remote_copy(
            src_ref=value_ref,
            dst_ref=slots.at[me],
            send_sem=send_sem.at[step],
            recv_sem=recv_sem.at[step],
            device_id={axis: peer},
            device_id_type=MESH,
        )
        copy.start()
        copies.append(copy)
    slots[me] = value_ref[...]
    for copy in copies:
        copy.wait()
    total = slots[0]
    for member in range(1, size):
        total = total + slots[member]
    total_ref[...] = total


def exchange_sum(value, axis, ident):
    size = lax.axis_size(axis)
    return pl.pallas_call(
        functools.partial(exchange_kernel, axis, size),
        out_shape=jax.ShapeDtypeStruct(value.shape, value.dtype),
        in_specs=[pl.BlockSpec(memory_space=pltpu.VMEM)],
        out_specs=pl.BlockSpec(memory_space=pltpu.VMEM),
        scratch_shapes=[
            pltpu.VMEM((size,) + value.shape, value.dtype),
            pltpu.SemaphoreType.DMA((size,)),
            pltpu.SemaphoreType.DMA((size,)),
        ],
        compiler_params=pltpu.CompilerParams(collective_id=ident, has_side_effects=True),
        name="exchange_" + str(ident),
    )(value)


def weight_kernel(starts, stride, grad_one, flat_in, grad_two, shifted, hidden_two, grad_three, out_ref):
    at = pl.program_id(0)
    rows = grad_two.shape[0]

    @pl.when(at < starts[0])
    def _():
        out_ref[...] = contract(grad_one[...], flat_in[...], 0, 0)

    @pl.when(jnp.logical_and(at >= starts[0], at < starts[1]))
    def _():
        tap = at - starts[0]
        first = pl.multiple_of((tap // 3) * stride, 16)
        window = shifted[lax.rem(tap, 3), pl.ds(first, rows), :]
        out_ref[...] = contract(grad_two[...], window, 0, 0)

    @pl.when(at >= starts[1])
    def _():
        out_ref[...] = contract(hidden_two[...], grad_three[...], 0, 0)


def weight_products(grad_one, flat_in, grad_two, shifted, hidden_two, grad_three):
    rows, mid = grad_one.shape
    stride = (shifted.shape[1] - rows) // 2
    counts = [flat_in.shape[1] // mid, 9, grad_three.shape[1] // mid]
    starts = (counts[0], counts[0] + counts[1])
    whole = pl.BlockSpec((rows, mid), lambda at: (0, 0))

    def columns(first, count):
        return pl.BlockSpec((rows, mid), lambda at: (0, jnp.clip(at - first, 0, count - 1)))

    return pl.pallas_call(
        functools.partial(weight_kernel, starts, stride),
        grid=(sum(counts),),
        out_shape=jax.ShapeDtypeStruct((mid, sum(counts) * mid), jnp.float32),
        in_specs=[
            whole,
            columns(0, counts[0]),
            whole,
            pl.BlockSpec(shifted.shape, lambda at: (0, 0, 0)),
            whole,
            columns(starts[1], counts[2]),
        ],
        out_specs=pl.BlockSpec((mid, mid), lambda at: (0, at)),
        name="weight_products",
    )(grad_one, flat_in, grad_two, shifted, hidden_two, grad_three)


def conv_kernel(mirror, width, padded, field, weights, out_ref, shifted):
    rows, mid = field.shape
    stride = (shifted.shape[1] - rows) // 2
    values = field[...].astype(jnp.float32)
    for col_tap in range(3):
        moved = values if col_tap == 1 else pltpu.roll(values, (1 - col_tap) % rows, 0)
        shifted[col_tap, :stride, :] = jnp.zeros((stride, mid), shifted.dtype)
        shifted[col_tap, stride + rows :, :] = jnp.zeros((stride, mid), shifted.dtype)
        shifted[col_tap, stride : stride + rows, :] = moved.astype(shifted.dtype)
    out_ref[...] = jnp.zeros_like(out_ref)

    def step(tap, carry):
        row_tap, col_tap = tap // 3, lax.rem(tap, 3)
        if mirror:
            row_tap, col_tap = 2 - row_tap, 2 - col_tap
        window = shifted[col_tap, pl.ds(pl.multiple_of(row_tap * stride, 16), rows), :]
        block = weights[pl.ds(pl.multiple_of(tap * mid, 16), mid), :]
        out_ref[...] += contract(window, block, 1, 1 if mirror else 0)
        return carry

    lax.fori_loop(0, 9, step, 0)
    column = lax.rem(lax.broadcasted_iota(jnp.int32, (rows, mid), 0), padded)
    out_ref[...] = jnp.where(column < width, out_ref[...], 0.0)


def convolve(field, weights, images_count, width, padded, mirror):
    rows, mid = field.shape
    stride = images_count * padded
    return pl.pallas_call(
        functools.partial(conv_kernel, mirror, width, padded),
        out_shape=(
            jax.ShapeDtypeStruct((rows, mid), jnp.float32),
            jax.ShapeDtypeStruct((3, rows + 2 * stride, mid), field.dtype),
        ),
        in_specs=[pl.BlockSpec(memory_space=pltpu.VMEM)] * 2,
        out_specs=[pl.BlockSpec(memory_space=pltpu.VMEM)] * 2,
        compiler_params=pltpu.CompilerParams(vmem_limit_bytes=40 * 1024 * 1024),
        name="convolve_back" if mirror else "convolve",
    )(field, weights)


def scatter_plan(n_group, n_rep, rows):
    bits = [("rep", at) for at in range(n_rep.bit_length() - 1)]
    bits += [("bngroup", at) for at in range(n_group.bit_length() - 1)]
    rest = len(bits) - 1
    near = list(range(rest))
    rep_rest = n_rep.bit_length() - 2
    orders = [
        near,
        near[1:rep_rest] + near[rep_rest:] + near[:1],
        near[rep_rest:] + near[:rep_rest],
    ]
    tiles = rows // 8
    sizes = [(tiles + 2) // 3, (tiles + 1) // 3, tiles // 3]
    streams, begin = [], 0
    for order, size in zip(orders, sizes):
        if size:
            streams.append((begin * 8, size * 8, order))
        begin += size
    return bits, streams


def scatter_kernel(n_group, n_rep, scale, grads, out_ref, own, got, load_sem, send_sem, recv_sem):
    rows, cols = out_ref.shape
    bits, streams = scatter_plan(n_group, n_rep, rows)
    rest = bits[1:]
    place = {"rep": lax.axis_index("rep"), "bngroup": lax.axis_index("bngroup")}

    def flipped(value, at):
        bit = lax.rem(value // (1 << at), 2)
        return value + (1 - 2 * bit) * (1 << at)

    def partner(axis, at):
        return {axis: flipped(place[axis], at)}

    barrier = pltpu.get_barrier_semaphore()
    for axis, at in bits:
        pl.semaphore_signal(barrier, inc=1, device_id=partner(axis, at), device_id_type=MESH)

    def source(relative, other, begin, size):
        spot = dict(place)
        for index, (axis, at) in enumerate(rest):
            if relative >> index & 1:
                spot[axis] = flipped(spot[axis], at)
        if other:
            spot["rep"] = flipped(spot["rep"], 0)
        first = pl.multiple_of(spot["rep"] * rows + begin, 8)
        if len(grads.shape) == 3:
            return grads.at[spot["bngroup"], pl.ds(first, size), :]
        return grads.at[pl.ds(first, size), pl.ds(pl.multiple_of(spot["bngroup"] * cols, 128), cols)]

    count = 1 << len(rest)
    slot_of, slots = {}, count
    for number, (begin, size, order) in enumerate(streams):
        used = count
        active = list(range(count))
        for stage, bit in enumerate(order):
            active = [relative for relative in active if not relative >> bit & 1]
            for relative in active:
                slot_of[number, stage, relative] = used
                used += 1

    def first_order(order):
        ranks = sorted(range(count), key=lambda rel: tuple(-(rel >> bit & 1) for bit in order))
        return ranks

    loads = {}
    for number, (begin, size, order) in enumerate(streams):
        for relative in range(count):
            copy = pltpu.make_async_copy(
                source(relative, False, begin, size),
                own.at[relative, pl.ds(begin, size), :],
                load_sem.at[number, relative],
            )
            loads[number, relative] = copy
    for relative in range(count):
        for number, (begin, size, order) in enumerate(streams):
            loads[number, first_order(order)[relative]].start()
    pl.semaphore_wait(barrier, len(bits))
    sent = []
    arrivals = {}
    for relative in range(count):
        for number, (begin, size, order) in enumerate(streams):
            which = first_order(order)[relative]
            copy = pltpu.make_async_remote_copy(
                src_ref=source(which, True, begin, size),
                dst_ref=got.at[which, pl.ds(begin, size), :],
                send_sem=send_sem.at[number, which],
                recv_sem=recv_sem.at[number, which],
                device_id=partner(*bits[0]),
                device_id_type=MESH,
            )
            copy.start()
            sent.append(copy)
            arrivals[number, -1, which] = copy

    def onward(number, stage, relative):
        begin, size, order = streams[number]
        bit = order[stage]
        slot = slot_of[number, stage, relative & ~(1 << bit)]
        copy = pltpu.make_async_remote_copy(
            src_ref=own.at[relative, pl.ds(begin, size), :],
            dst_ref=got.at[slot, pl.ds(begin, size), :],
            send_sem=send_sem.at[number, slot],
            recv_sem=recv_sem.at[number, slot],
            device_id=partner(*rest[bit]),
            device_id_type=MESH,
        )
        copy.start()
        sent.append(copy)
        arrivals[number, stage, relative & ~(1 << bit)] = copy

    pending = []
    for stage in range(-1, len(rest)):
        active = []
        for number, (begin, size, order) in enumerate(streams):
            done = 0
            for bit in order[: stage + 1]:
                done |= 1 << bit
            active.append([rel for rel in first_order(order) if not rel & done])
        for position in range(len(active[0])):
            for number, (begin, size, order) in enumerate(streams):
                relative = active[number][position]
                slot = relative if stage < 0 else slot_of[number, stage, relative]
                if stage < 0:
                    loads[number, relative].wait()
                arrivals[number, stage, relative].wait_recv()
                window = pl.ds(begin, size)
                total = own[relative, window, :] + got[slot, window, :]
                if stage == len(rest) - 1:
                    out_ref[window, :] = total * scale
                else:
                    own[relative, window, :] = total
                while pending:
                    onward(*pending.pop(0))
                if stage + 1 < len(rest) and relative >> order[stage + 1] & 1:
                    pending.append((number, stage + 1, relative))
        while pending:
            onward(*pending.pop(0))
    for copy in sent:
        copy.wait_send()


def scatter_sum(grads, images_total, ident):
    n_group, n_rep = lax.axis_size("bngroup"), lax.axis_size("rep")
    rows, cols = grads.shape[0] // n_rep, grads.shape[1] // n_group
    if cols % 128:
        grads = grads.reshape(grads.shape[0], n_group, cols).transpose(1, 0, 2)
    bits, streams = scatter_plan(n_group, n_rep, rows)
    count = 1 << (len(bits) - 1)
    held = 2 * count - 1
    return pl.pallas_call(
        functools.partial(scatter_kernel, n_group, n_rep, 1.0 / images_total),
        out_shape=jax.ShapeDtypeStruct((rows, cols), jnp.float32),
        in_specs=[pl.BlockSpec(memory_space=pl.ANY)],
        out_specs=pl.BlockSpec(memory_space=pltpu.VMEM),
        scratch_shapes=[
            pltpu.VMEM((count, rows, cols), jnp.float32),
            pltpu.VMEM((held, rows, cols), jnp.float32),
            pltpu.SemaphoreType.DMA((len(streams), count)),
            pltpu.SemaphoreType.DMA((len(streams), held)),
            pltpu.SemaphoreType.DMA((len(streams), held)),
        ],
        compiler_params=pltpu.CompilerParams(
            collective_id=ident, has_side_effects=True, vmem_limit_bytes=60 * 1024 * 1024
        ),
        name="scatter_sum",
    )(grads)


def slope(value):
    sigma = jax.nn.sigmoid(value)
    return sigma * (1.0 + value * (1.0 - sigma))


def normalize(pre_norm, norm_gain, norm_shift, number, ident):
    sums = jnp.stack([jnp.sum(pre_norm, axis=0), jnp.sum(pre_norm * pre_norm, axis=0)])
    first_sum, second_sum = exchange_sum(sums, "bngroup", ident)
    centre = first_sum / number
    spread = jnp.maximum(second_sum / number - centre * centre, 0.0)
    inverse = lax.rsqrt(spread + EPS)
    scaled = (pre_norm - centre) * inverse
    return (scaled, inverse, norm_gain * scaled + norm_shift)


def norm_back(upstream, scaled, inverse, norm_gain, real, number, ident):
    sums = jnp.stack([jnp.sum(upstream, axis=0), jnp.sum(upstream * scaled, axis=0)])
    shift_sum, gain_sum = exchange_sum(sums, "bngroup", ident)
    result = norm_gain * inverse * (upstream - shift_sum / number - scaled * gain_sum / number)
    result = jnp.where(real, result, 0.0)
    return (result.astype(jnp.bfloat16), shift_sum, gain_sum)


def to_rows(field, padded):
    turned = field.transpose(1, 0, 2, 3)
    turned = jnp.pad(turned, ((0, 0), (0, 0), (0, padded - field.shape[2]), (0, 0)))
    return turned.reshape(-1, field.shape[3])


def from_rows(rows, shape, padded):
    turned = rows.reshape(shape[1], shape[0], padded, shape[3])
    return turned[:, :, : shape[2], :].transpose(1, 0, 2, 3)


def per_device(images, cotangent, w_reduce, w_spatial, w_expand, norm_gain, norm_shift):
    group_size = lax.axis_size("bngroup")
    images_total = images.shape[0] * group_size * lax.axis_size("rep")
    images_count = images.shape[0]
    length = images.shape[1]
    wide_ch = images.shape[3]
    mid_ch = w_reduce.shape[1]
    padded = (images.shape[2] // 8 + 1) * 8
    number = images_count * length * images.shape[2] * group_size
    flat_in = to_rows(images, padded)
    real = (jnp.arange(flat_in.shape[0]) % padded < images.shape[2])[:, None]
    gain_one, gain_two, gain_three = (
        norm_gain[:mid_ch],
        norm_gain[mid_ch : 2 * mid_ch],
        norm_gain[2 * mid_ch :],
    )
    shift_one, shift_two, shift_three = (
        norm_shift[:mid_ch],
        norm_shift[mid_ch : 2 * mid_ch],
        norm_shift[2 * mid_ch :],
    )
    scaled_one, inverse_one, normed_one = normalize(
        matmul(flat_in, w_reduce), gain_one, shift_one, number, 0
    )
    hidden_one = jnp.where(real, jax.nn.silu(normed_one), 0.0).astype(jnp.bfloat16)
    spatial_pre, shifted = convolve(
        hidden_one, w_spatial, images_count, images.shape[2], padded, False
    )
    scaled_two, inverse_two, normed_two = normalize(
        spatial_pre, gain_two, shift_two, number, 1
    )
    hidden_two = jnp.where(real, jax.nn.silu(normed_two), 0.0).astype(jnp.bfloat16)
    scaled_three, inverse_three, normed_three = normalize(
        contract(hidden_two, w_expand, 1, 1), gain_three, shift_three, number, 2
    )
    summed_in = normed_three + flat_in.astype(jnp.float32)
    output = jax.nn.silu(summed_in).astype(jnp.bfloat16)
    upstream = to_rows(cotangent, padded).astype(jnp.float32) * slope(summed_in)
    grad_three, shift_sum_three, gain_sum_three = norm_back(
        upstream, scaled_three, inverse_three, gain_three, real, number, 3
    )
    back_two = matmul(grad_three, w_expand) * slope(normed_two)
    grad_two, shift_sum_two, gain_sum_two = norm_back(
        back_two, scaled_two, inverse_two, gain_two, real, number, 4
    )
    spatial_back, _ = convolve(grad_two, w_spatial, images_count, images.shape[2], padded, True)
    back_one = spatial_back * slope(normed_one)
    grad_one, shift_sum_one, gain_sum_one = norm_back(
        back_one, scaled_one, inverse_one, gain_one, real, number, 5
    )
    in_grad = (upstream + contract(grad_one, w_reduce, 1, 1)).astype(jnp.bfloat16)
    local_grads = weight_products(
        grad_one, flat_in, grad_two, shifted, hidden_two, grad_three
    )
    summed_grads = scatter_sum(local_grads, images_total, 7).T
    group_norms = jnp.stack(
        [
            jnp.concatenate([gain_sum_one, gain_sum_two, gain_sum_three]),
            jnp.concatenate([shift_sum_one, shift_sum_two, shift_sum_three]),
        ]
    )
    norm_summed = exchange_sum(group_norms, "rep", 6)
    return (
        from_rows(output, images.shape, padded),
        from_rows(in_grad, images.shape, padded),
        summed_grads,
        norm_summed / images_total,
    )


def solution(mesh):
    in_specs = (
        P(("bngroup", "rep"), None, None, None),
        P(("bngroup", "rep"), None, None, None),
        P(),
        P(),
        P(),
        P(),
        P(),
    )
    out_specs = (
        P(("bngroup", "rep"), None, None, None),
        P(("bngroup", "rep"), None, None, None),
        P("bngroup", "rep"),
        P(),
    )
    return jax.shard_map(
        per_device, mesh=mesh, in_specs=in_specs, out_specs=out_specs, check_vma=False
    )
```

```python
import functools

import jax
import jax.numpy as jnp
from jax import lax
from jax.experimental import pallas as pl
from jax.experimental.pallas import tpu as pltpu
from jax.sharding import PartitionSpec as P

MESH = pl.DeviceIdType.MESH

EPS = 0.25


def matmul(left, right):
    return jnp.dot(left, right, preferred_element_type=jnp.float32)


def contract(left, right, left_dim, right_dim):
    return lax.dot_general(
        left, right, (((left_dim,), (right_dim,)), ((), ())), preferred_element_type=jnp.float32
    )


def exchange_kernel(axis, size, value_ref, total_ref, slots, send_sem, recv_sem):
    me = lax.axis_index(axis)
    barrier = pltpu.get_barrier_semaphore()
    for step in range(1, size):
        peer = lax.rem(me + step, size)
        pl.semaphore_signal(barrier, inc=1, device_id={axis: peer}, device_id_type=MESH)
    pl.semaphore_wait(barrier, size - 1)
    copies = []
    for step in range(1, size):
        peer = lax.rem(me + step, size)
        copy = pltpu.make_async_remote_copy(
            src_ref=value_ref,
            dst_ref=slots.at[me],
            send_sem=send_sem.at[step],
            recv_sem=recv_sem.at[step],
            device_id={axis: peer},
            device_id_type=MESH,
        )
        copy.start()
        copies.append(copy)
    slots[me] = value_ref[...]
    for copy in copies:
        copy.wait()
    total = slots[0]
    for member in range(1, size):
        total = total + slots[member]
    total_ref[...] = total


def exchange_sum(value, axis, ident):
    size = lax.axis_size(axis)
    return pl.pallas_call(
        functools.partial(exchange_kernel, axis, size),
        out_shape=jax.ShapeDtypeStruct(value.shape, value.dtype),
        in_specs=[pl.BlockSpec(memory_space=pltpu.VMEM)],
        out_specs=pl.BlockSpec(memory_space=pltpu.VMEM),
        scratch_shapes=[
            pltpu.VMEM((size,) + value.shape, value.dtype),
            pltpu.SemaphoreType.DMA((size,)),
            pltpu.SemaphoreType.DMA((size,)),
        ],
        compiler_params=pltpu.CompilerParams(collective_id=ident, has_side_effects=True),
        name="exchange_" + str(ident),
    )(value)


def weight_kernel(starts, stride, grad_one, flat_in, grad_two, shifted, hidden_two, grad_three, out_ref):
    at = pl.program_id(0)
    rows = grad_two.shape[0]

    @pl.when(at < starts[0])
    def _():
        out_ref[...] = contract(grad_one[...], flat_in[...], 0, 0)

    @pl.when(jnp.logical_and(at >= starts[0], at < starts[1]))
    def _():
        tap = at - starts[0]
        first = pl.multiple_of((tap // 3) * stride, 16)
        window = shifted[lax.rem(tap, 3), pl.ds(first, rows), :]
        out_ref[...] = contract(grad_two[...], window, 0, 0)

    @pl.when(at >= starts[1])
    def _():
        out_ref[...] = contract(hidden_two[...], grad_three[...], 0, 0)


def weight_products(grad_one, flat_in, grad_two, shifted, hidden_two, grad_three):
    rows, mid = grad_one.shape
    stride = (shifted.shape[1] - rows) // 2
    counts = [flat_in.shape[1] // mid, 9, grad_three.shape[1] // mid]
    starts = (counts[0], counts[0] + counts[1])
    whole = pl.BlockSpec((rows, mid), lambda at: (0, 0))

    def columns(first, count):
        return pl.BlockSpec((rows, mid), lambda at: (0, jnp.clip(at - first, 0, count - 1)))

    return pl.pallas_call(
        functools.partial(weight_kernel, starts, stride),
        grid=(sum(counts),),
        out_shape=jax.ShapeDtypeStruct((mid, sum(counts) * mid), jnp.float32),
        in_specs=[
            whole,
            columns(0, counts[0]),
            whole,
            pl.BlockSpec(shifted.shape, lambda at: (0, 0, 0)),
            whole,
            columns(starts[1], counts[2]),
        ],
        out_specs=pl.BlockSpec((mid, mid), lambda at: (0, at)),
        name="weight_products",
    )(grad_one, flat_in, grad_two, shifted, hidden_two, grad_three)


def conv_kernel(mirror, width, padded, field, weights, out_ref, shifted):
    rows, mid = field.shape
    stride = (shifted.shape[1] - rows) // 2
    values = field[...].astype(jnp.float32)
    for col_tap in range(3):
        moved = values if col_tap == 1 else pltpu.roll(values, (1 - col_tap) % rows, 0)
        shifted[col_tap, :stride, :] = jnp.zeros((stride, mid), shifted.dtype)
        shifted[col_tap, stride + rows :, :] = jnp.zeros((stride, mid), shifted.dtype)
        shifted[col_tap, stride : stride + rows, :] = moved.astype(shifted.dtype)
    out_ref[...] = jnp.zeros_like(out_ref)

    def step(tap, carry):
        row_tap, col_tap = tap // 3, lax.rem(tap, 3)
        if mirror:
            row_tap, col_tap = 2 - row_tap, 2 - col_tap
        window = shifted[col_tap, pl.ds(pl.multiple_of(row_tap * stride, 16), rows), :]
        block = weights[pl.ds(pl.multiple_of(tap * mid, 16), mid), :]
        out_ref[...] += contract(window, block, 1, 1 if mirror else 0)
        return carry

    lax.fori_loop(0, 9, step, 0)
    column = lax.rem(lax.broadcasted_iota(jnp.int32, (rows, mid), 0), padded)
    out_ref[...] = jnp.where(column < width, out_ref[...], 0.0)


def convolve(field, weights, images_count, width, padded, mirror):
    rows, mid = field.shape
    stride = images_count * padded
    return pl.pallas_call(
        functools.partial(conv_kernel, mirror, width, padded),
        out_shape=(
            jax.ShapeDtypeStruct((rows, mid), jnp.float32),
            jax.ShapeDtypeStruct((3, rows + 2 * stride, mid), field.dtype),
        ),
        in_specs=[pl.BlockSpec(memory_space=pltpu.VMEM)] * 2,
        out_specs=[pl.BlockSpec(memory_space=pltpu.VMEM)] * 2,
        compiler_params=pltpu.CompilerParams(vmem_limit_bytes=40 * 1024 * 1024),
        name="convolve_back" if mirror else "convolve",
    )(field, weights)


def scatter_plan(n_group, n_rep, rows):
    bits = [("rep", at) for at in range(n_rep.bit_length() - 1)]
    bits += [("bngroup", at) for at in range(n_group.bit_length() - 1)]
    rest = len(bits) - 1
    near = list(range(rest))
    rep_rest = n_rep.bit_length() - 2
    orders = [
        near,
        near[1:rep_rest] + near[rep_rest:] + near[:1],
        near[rep_rest:] + near[:rep_rest],
    ]
    tiles = rows // 8
    sizes = [(tiles + 2) // 3, (tiles + 1) // 3, tiles // 3]
    streams, begin = [], 0
    for order, size in zip(orders, sizes):
        if size:
            streams.append((begin * 8, size * 8, order))
        begin += size
    return bits, streams


def scatter_kernel(
    n_group, n_rep, scale, grads, norms, out_ref, norm_out, own, got, load_sem, send_sem, recv_sem, slots, far_send, far_recv
):
    rows, cols = out_ref.shape
    bits, streams = scatter_plan(n_group, n_rep, rows)
    rest = bits[1:]
    place = {"rep": lax.axis_index("rep"), "bngroup": lax.axis_index("bngroup")}

    def flipped(value, at):
        bit = lax.rem(value // (1 << at), 2)
        return value + (1 - 2 * bit) * (1 << at)

    def partner(axis, at):
        return {axis: flipped(place[axis], at)}

    barrier = pltpu.get_barrier_semaphore()
    for axis, at in bits:
        pl.semaphore_signal(barrier, inc=1, device_id=partner(axis, at), device_id_type=MESH)
    peers = [lax.rem(place["rep"] + step, n_rep) for step in range(1, n_rep)]
    for peer in peers:
        pl.semaphore_signal(barrier, inc=1, device_id={"rep": peer}, device_id_type=MESH)

    def source(relative, other, begin, size):
        spot = dict(place)
        for index, (axis, at) in enumerate(rest):
            if relative >> index & 1:
                spot[axis] = flipped(spot[axis], at)
        if other:
            spot["rep"] = flipped(spot["rep"], 0)
        first = pl.multiple_of(spot["rep"] * rows + begin, 8)
        if len(grads.shape) == 3:
            return grads.at[spot["bngroup"], pl.ds(first, size), :]
        return grads.at[pl.ds(first, size), pl.ds(pl.multiple_of(spot["bngroup"] * cols, 128), cols)]

    count = 1 << len(rest)
    slot_of = {}
    for number, (begin, size, order) in enumerate(streams):
        used = count
        active = list(range(count))
        for stage, bit in enumerate(order):
            active = [relative for relative in active if not relative >> bit & 1]
            for relative in active:
                slot_of[number, stage, relative] = used
                used += 1

    def first_order(order):
        ranks = sorted(range(count), key=lambda rel: tuple(-(rel >> bit & 1) for bit in order))
        return ranks

    loads = {}
    for number, (begin, size, order) in enumerate(streams):
        for relative in range(count):
            copy = pltpu.make_async_copy(
                source(relative, False, begin, size),
                own.at[relative, pl.ds(begin, size), :],
                load_sem.at[number, relative],
            )
            loads[number, relative] = copy
    for relative in range(count):
        for number, (begin, size, order) in enumerate(streams):
            loads[number, first_order(order)[relative]].start()
    pl.semaphore_wait(barrier, len(bits) + n_rep - 1)
    far = []
    for step, peer in enumerate(peers):
        copy = pltpu.make_async_remote_copy(
            src_ref=norms,
            dst_ref=slots.at[place["rep"]],
            send_sem=far_send.at[step],
            recv_sem=far_recv.at[step],
            device_id={"rep": peer},
            device_id_type=MESH,
        )
        copy.start()
        far.append(copy)
    slots[place["rep"]] = norms[...]
    sent = []
    arrivals = {}
    for relative in range(count):
        for number, (begin, size, order) in enumerate(streams):
            which = first_order(order)[relative]
            copy = pltpu.make_async_remote_copy(
                src_ref=source(which, True, begin, size),
                dst_ref=got.at[which, pl.ds(begin, size), :],
                send_sem=send_sem.at[number, which],
                recv_sem=recv_sem.at[number, which],
                device_id=partner(*bits[0]),
                device_id_type=MESH,
            )
            copy.start()
            sent.append(copy)
            arrivals[number, -1, which] = copy

    def onward(number, stage, relative):
        begin, size, order = streams[number]
        bit = order[stage]
        slot = slot_of[number, stage, relative & ~(1 << bit)]
        copy = pltpu.make_async_remote_copy(
            src_ref=own.at[relative, pl.ds(begin, size), :],
            dst_ref=got.at[slot, pl.ds(begin, size), :],
            send_sem=send_sem.at[number, slot],
            recv_sem=recv_sem.at[number, slot],
            device_id=partner(*rest[bit]),
            device_id_type=MESH,
        )
        copy.start()
        sent.append(copy)
        arrivals[number, stage, relative & ~(1 << bit)] = copy

    pending = []
    for stage in range(-1, len(rest)):
        active = []
        for number, (begin, size, order) in enumerate(streams):
            done = 0
            for bit in order[: stage + 1]:
                done |= 1 << bit
            active.append([rel for rel in first_order(order) if not rel & done])
        for position in range(len(active[0])):
            for number, (begin, size, order) in enumerate(streams):
                relative = active[number][position]
                slot = relative if stage < 0 else slot_of[number, stage, relative]
                if stage < 0:
                    loads[number, relative].wait()
                arrivals[number, stage, relative].wait_recv()
                window = pl.ds(begin, size)
                total = own[relative, window, :] + got[slot, window, :]
                if stage == len(rest) - 1:
                    out_ref[window, :] = total * scale
                else:
                    own[relative, window, :] = total
                while pending:
                    onward(*pending.pop(0))
                if stage + 1 < len(rest) and relative >> order[stage + 1] & 1:
                    pending.append((number, stage + 1, relative))
        while pending:
            onward(*pending.pop(0))
    for copy in sent:
        copy.wait_send()
    for copy in far:
        copy.wait()
    total = slots[0]
    for member in range(1, n_rep):
        total = total + slots[member]
    norm_out[...] = total * scale


def scatter_sum(grads, norms, images_total, ident):
    n_group, n_rep = lax.axis_size("bngroup"), lax.axis_size("rep")
    rows, cols = grads.shape[0] // n_rep, grads.shape[1] // n_group
    if cols % 128:
        grads = grads.reshape(grads.shape[0], n_group, cols).transpose(1, 0, 2)
    bits, streams = scatter_plan(n_group, n_rep, rows)
    count = 1 << (len(bits) - 1)
    held = 2 * count - 1
    return pl.pallas_call(
        functools.partial(scatter_kernel, n_group, n_rep, 1.0 / images_total),
        out_shape=(
            jax.ShapeDtypeStruct((rows, cols), jnp.float32),
            jax.ShapeDtypeStruct(norms.shape, jnp.float32),
        ),
        in_specs=[pl.BlockSpec(memory_space=pl.ANY), pl.BlockSpec(memory_space=pltpu.VMEM)],
        out_specs=[pl.BlockSpec(memory_space=pltpu.VMEM)] * 2,
        scratch_shapes=[
            pltpu.VMEM((count, rows, cols), jnp.float32),
            pltpu.VMEM((held, rows, cols), jnp.float32),
            pltpu.SemaphoreType.DMA((len(streams), count)),
            pltpu.SemaphoreType.DMA((len(streams), held)),
            pltpu.SemaphoreType.DMA((len(streams), held)),
            pltpu.VMEM((n_rep,) + norms.shape, jnp.float32),
            pltpu.SemaphoreType.DMA((n_rep,)),
            pltpu.SemaphoreType.DMA((n_rep,)),
        ],
        compiler_params=pltpu.CompilerParams(
            collective_id=ident, has_side_effects=True, vmem_limit_bytes=60 * 1024 * 1024
        ),
        name="scatter_sum",
    )(grads, norms)


def slope(value):
    sigma = jax.nn.sigmoid(value)
    return sigma * (1.0 + value * (1.0 - sigma))


def normalize(pre_norm, norm_gain, norm_shift, number, ident):
    sums = jnp.stack([jnp.sum(pre_norm, axis=0), jnp.sum(pre_norm * pre_norm, axis=0)])
    first_sum, second_sum = exchange_sum(sums, "bngroup", ident)
    centre = first_sum / number
    spread = jnp.maximum(second_sum / number - centre * centre, 0.0)
    inverse = lax.rsqrt(spread + EPS)
    scaled = (pre_norm - centre) * inverse
    return (scaled, inverse, norm_gain * scaled + norm_shift)


def norm_back(upstream, scaled, inverse, norm_gain, real, number, ident):
    sums = jnp.stack([jnp.sum(upstream, axis=0), jnp.sum(upstream * scaled, axis=0)])
    shift_sum, gain_sum = exchange_sum(sums, "bngroup", ident)
    result = norm_gain * inverse * (upstream - shift_sum / number - scaled * gain_sum / number)
    result = jnp.where(real, result, 0.0)
    return (result.astype(jnp.bfloat16), shift_sum, gain_sum)


def to_rows(field, padded):
    turned = field.transpose(1, 0, 2, 3)
    turned = jnp.pad(turned, ((0, 0), (0, 0), (0, padded - field.shape[2]), (0, 0)))
    return turned.reshape(-1, field.shape[3])


def from_rows(rows, shape, padded):
    turned = rows.reshape(shape[1], shape[0], padded, shape[3])
    return turned[:, :, : shape[2], :].transpose(1, 0, 2, 3)


def per_device(images, cotangent, w_reduce, w_spatial, w_expand, norm_gain, norm_shift):
    group_size = lax.axis_size("bngroup")
    images_total = images.shape[0] * group_size * lax.axis_size("rep")
    images_count = images.shape[0]
    length = images.shape[1]
    wide_ch = images.shape[3]
    mid_ch = w_reduce.shape[1]
    padded = (images.shape[2] // 8 + 1) * 8
    number = images_count * length * images.shape[2] * group_size
    flat_in = to_rows(images, padded)
    real = (jnp.arange(flat_in.shape[0]) % padded < images.shape[2])[:, None]
    gain_one, gain_two, gain_three = (
        norm_gain[:mid_ch],
        norm_gain[mid_ch : 2 * mid_ch],
        norm_gain[2 * mid_ch :],
    )
    shift_one, shift_two, shift_three = (
        norm_shift[:mid_ch],
        norm_shift[mid_ch : 2 * mid_ch],
        norm_shift[2 * mid_ch :],
    )
    scaled_one, inverse_one, normed_one = normalize(
        matmul(flat_in, w_reduce), gain_one, shift_one, number, 0
    )
    hidden_one = jnp.where(real, jax.nn.silu(normed_one), 0.0).astype(jnp.bfloat16)
    spatial_pre, shifted = convolve(
        hidden_one, w_spatial, images_count, images.shape[2], padded, False
    )
    scaled_two, inverse_two, normed_two = normalize(
        spatial_pre, gain_two, shift_two, number, 1
    )
    hidden_two = jnp.where(real, jax.nn.silu(normed_two), 0.0).astype(jnp.bfloat16)
    scaled_three, inverse_three, normed_three = normalize(
        contract(hidden_two, w_expand, 1, 1), gain_three, shift_three, number, 2
    )
    summed_in = normed_three + flat_in.astype(jnp.float32)
    output = jax.nn.silu(summed_in).astype(jnp.bfloat16)
    upstream = to_rows(cotangent, padded).astype(jnp.float32) * slope(summed_in)
    grad_three, shift_sum_three, gain_sum_three = norm_back(
        upstream, scaled_three, inverse_three, gain_three, real, number, 3
    )
    back_two = matmul(grad_three, w_expand) * slope(normed_two)
    grad_two, shift_sum_two, gain_sum_two = norm_back(
        back_two, scaled_two, inverse_two, gain_two, real, number, 4
    )
    spatial_back, _ = convolve(grad_two, w_spatial, images_count, images.shape[2], padded, True)
    back_one = spatial_back * slope(normed_one)
    grad_one, shift_sum_one, gain_sum_one = norm_back(
        back_one, scaled_one, inverse_one, gain_one, real, number, 5
    )
    in_grad = (upstream + contract(grad_one, w_reduce, 1, 1)).astype(jnp.bfloat16)
    local_grads = weight_products(
        grad_one, flat_in, grad_two, shifted, hidden_two, grad_three
    )
    group_norms = jnp.stack(
        [
            jnp.concatenate([gain_sum_one, gain_sum_two, gain_sum_three]),
            jnp.concatenate([shift_sum_one, shift_sum_two, shift_sum_three]),
        ]
    )
    summed_grads, norm_summed = scatter_sum(local_grads, group_norms, images_total, 7)
    return (
        from_rows(output, images.shape, padded),
        from_rows(in_grad, images.shape, padded),
        summed_grads.T,
        norm_summed,
    )


def solution(mesh):
    in_specs = (
        P(("bngroup", "rep"), None, None, None),
        P(("bngroup", "rep"), None, None, None),
        P(),
        P(),
        P(),
        P(),
        P(),
    )
    out_specs = (
        P(("bngroup", "rep"), None, None, None),
        P(("bngroup", "rep"), None, None, None),
        P("bngroup", "rep"),
        P(),
    )
    return jax.shard_map(
        per_device, mesh=mesh, in_specs=in_specs, out_specs=out_specs, check_vma=False
    )
```
